16 devices in a mesh: dp: 4 (over y, z, core), sp: 4 (over x).
Axes of the slice: x: 4, y: 2, z: 1, core: 2. Of those that a mesh axis runs over, the one named last changes fastest.
The devices are a block of a 4x4x8 slice.
Arguments:
- x: bfloat16 [32768, 2560], P(('dp', 'sp')), parts along dimension 0
- gain: bfloat16 [2560], replicated
- wq: bfloat16 [2560, 2048], P('sp')
- wk: bfloat16 [2560, 1024], P('sp')
- wv: bfloat16 [2560, 1024], P('sp')
- wo: bfloat16 [2048, 2560], P('sp')
Outputs:
- output: bfloat16 [32768, 2560], P(('dp', 'sp')), parts along dimension 0
There are 4 independent parts. The reference program is written for one: setup_inputs(seed, part) draws one part's arguments, and reference() takes and returns one part's arrays. A program takes and returns all parts, laid end to end along the dimension named above; an argument that names none is the same for every part.
All inputs are finite; a program needn't handle non-finite values.
Results may differ from the reference program's by a relative error of at most 0.012.
Values are sent between devices in bfloat16 or wider.
A program may use at most 768 MiB of HBM per device.

```python
import jax
import jax.numpy as jnp
from jax import lax

ROWS = 8192
D = 2560
HEADS = 8
KV_HEADS = 4
HEAD = 256
THETA = 10000


def setup_inputs(seed: int = 0, part: int = 0) -> dict:
    kx, kn, kq, kk, kv, ko = jax.random.split(jax.random.key(seed), 6)

    def weights(key, rows, columns):
        return jax.random.normal(key, (rows, columns), jnp.float32) * rows**-0.5

    drawn = {
        "x": jax.random.normal(jax.random.fold_in(kx, part), (ROWS, D), jnp.float32),
        "gain": 1 + 0.1 * jax.random.normal(kn, (D,), jnp.float32),
        "wq": 2 * weights(kq, D, HEADS * HEAD),
        "wk": 2 * weights(kk, D, KV_HEADS * HEAD),
        "wv": 4 * weights(kv, D, KV_HEADS * HEAD),
        "wo": weights(ko, HEADS * HEAD, D),
    }
    return {k: v.astype(jnp.bfloat16) for k, v in drawn.items()}


def normed(x, gain):
    wide = x.astype(jnp.float32)
    scale = lax.rsqrt(jnp.mean(wide * wide, -1, keepdims=True) + 1e-6)
    return (wide * scale * gain.astype(jnp.float32)).astype(jnp.bfloat16)


def turned(t, place, theta):
    half = t.shape[-1] // 2
    angle = place.astype(jnp.float32)[:, None] * theta ** (-jnp.arange(half, dtype=jnp.float32) / half)
    cos, sin = jnp.cos(angle)[:, None], jnp.sin(angle)[:, None]
    a, b = t[..., :half].astype(jnp.float32), t[..., half:].astype(jnp.float32)
    return jnp.concatenate([a * cos - b * sin, b * cos + a * sin], -1).astype(jnp.bfloat16)


def matmul(a, w):
    return jnp.dot(a, w, preferred_element_type=jnp.float32).astype(jnp.bfloat16)


def einsum(form, a, b):
    return jnp.einsum(form, a.astype(jnp.float32), b.astype(jnp.float32))


def attention(q, k, v):
    scores = einsum("tgsd,ugd->gstu", q, k) * q.shape[-1] ** -0.5
    token = jnp.arange(q.shape[0])
    scores = jnp.where(token[:, None] >= token, scores, -jnp.inf)
    weights = jax.nn.softmax(scores, -1).astype(jnp.bfloat16)
    return einsum("gstu,ugd->tgsd", weights, v).astype(jnp.bfloat16)


def reference(x, gain, wq, wk, wv, wo):
    a, place = normed(x, gain), jnp.arange(ROWS)
    q = turned(matmul(a, wq).reshape(ROWS, HEADS, HEAD), place, THETA).reshape(ROWS, KV_HEADS, -1, HEAD)
    k = turned(matmul(a, wk).reshape(ROWS, KV_HEADS, HEAD), place, THETA)
    v = matmul(a, wv).reshape(ROWS, KV_HEADS, HEAD)
    seen = attention(q, k, v).reshape(ROWS, HEADS * HEAD)
    return (x.astype(jnp.float32) + jnp.dot(seen, wo, preferred_element_type=jnp.float32)).astype(jnp.bfloat16)
```

```python
import functools

import jax
import jax.numpy as jnp
from jax import lax
from jax.experimental import pallas as pl
from jax.experimental.pallas import tpu as pltpu
from jax.sharding import PartitionSpec as P


NEG = -1e30
HIDDEN = 2 * NEG
LOG2E = 1.4426950408889634
VMEM = 56 * 2**20
HEAD = 256
THETA = 10000
STRIP = 512


def _dot(a, b, ca, cb):
    return lax.dot_general(a, b, (((ca,), (cb,)), ((), ())), preferred_element_type=jnp.float32)


def _assemble(off_ref, pieces, wbuf, sems):
    copies = []
    for n, piece in enumerate(pieces):
        rows = pl.ds(pl.multiple_of(off_ref[n], 32), piece.shape[0])
        copies.append(pltpu.make_async_copy(piece, wbuf.at[rows], sems.at[n]))
    for c in copies:
        c.start()
    for c in copies:
        c.wait()


def _project(off_ref, x_ref, gain_ref, cos_ref, sin_ref, *rest, pieces, outs, turn):
    w_refs, (out_ref, wbuf, a_s, sems) = rest[:pieces], rest[pieces:]

    @pl.when(pl.program_id(0) == 0)
    def _():
        _assemble(off_ref, w_refs, wbuf, sems)

    wide = x_ref[...].astype(jnp.float32)
    scale = lax.rsqrt(jnp.mean(wide * wide, -1, keepdims=True) + 1e-6)
    a_s[...] = (wide * scale * gain_ref[...].astype(jnp.float32)).astype(jnp.bfloat16)
    half = HEAD // 2
    per = out_ref.shape[1]
    for n in range(outs * per):
        t = _dot(a_s[...], wbuf[:, n * HEAD : (n + 1) * HEAD], 1, 0).astype(jnp.bfloat16)
        if turn[n % per]:
            a, b = t[:, :half].astype(jnp.float32), t[:, half:].astype(jnp.float32)
            cos, sin = cos_ref[...], sin_ref[...]
            t = jnp.concatenate([a * cos - b * sin, b * cos + a * sin], -1).astype(jnp.bfloat16)
        out_ref[n // per, n % per] = t


def project(x, gain, cos, sin, offsets, pieces, outs, turn, bm=256):
    own, d = x.shape
    n = pieces[0].shape[1]
    per = len(turn)
    row = lambda i, _: (i, 0)
    return pl.pallas_call(
        functools.partial(_project, pieces=len(pieces), outs=outs, turn=turn),
        grid_spec=pltpu.PrefetchScalarGridSpec(
            num_scalar_prefetch=1,
            grid=(own // bm,),
            in_specs=[pl.BlockSpec((bm, d), row), pl.BlockSpec((1, d), lambda i, _: (0, 0)), pl.BlockSpec((bm, HEAD // 2), row),
                      pl.BlockSpec((bm, HEAD // 2), row)] + [pl.BlockSpec(memory_space=pl.ANY)] * len(pieces),
            out_specs=pl.BlockSpec((outs, per, bm, HEAD), lambda i, _: (0, 0, i, 0)),
            scratch_shapes=[pltpu.VMEM((d, n), jnp.bfloat16), pltpu.VMEM((bm, d), jnp.bfloat16), pltpu.SemaphoreType.DMA((len(pieces),))],
        ),
        out_shape=jax.ShapeDtypeStruct((outs, per, own, HEAD), jnp.bfloat16),
        compiler_params=pltpu.CompilerParams(dimension_semantics=("arbitrary",), vmem_limit_bytes=VMEM),
        cost_estimate=pl.CostEstimate(flops=2 * own * d * n, transcendentals=0, bytes_accessed=2 * (own * d + d * n + own * n)),
    )(offsets, x, gain, cos, sin, *pieces)


MESH = pl.DeviceIdType.MESH


def _group(q_hbm, kv_hbm, seen_hbm, guest_hbm, far_hbm, kvs, qbuf, mix, top, obuf, lbuf, flse, kv_sem, load_sem, near_s, near_r, q_s, q_r,
           o_s, o_r, l_s, l_r, out_sem, *, scale, bk):
    heads, g, tokens, d = q_hbm.shape
    low = q_hbm.dtype
    e = scale * LOG2E
    cols = g * tokens
    wide = STRIP
    me = lax.axis_index("sp")
    size = lax.axis_size("sp")
    is_low, is_high, odd = me < 2, me >= 2, lax.rem(me, 2) == 1
    beside, opposite = me + 1 - 2 * lax.rem(me, 2), 3 - me

    barrier = pltpu.get_barrier_semaphore()
    for by in (1, size - 1):
        pl.semaphore_signal(barrier, inc=1, device_id={"sp": lax.rem(me + by, size)}, device_id_type=MESH)
    pl.semaphore_wait(barrier, 2)

    def near_copy(h):
        return pltpu.make_async_remote_copy(kv_hbm.at[h], kvs.at[heads + h], near_s.at[h], near_r.at[h], device_id={"sp": beside},
                                            device_id_type=MESH)

    def q_copy(h):
        return pltpu.make_async_remote_copy(q_hbm.at[h], guest_hbm.at[h], q_s.at[h], q_r.at[h], device_id={"sp": opposite},
                                            device_id_type=MESH)

    def o_copy(h):
        return pltpu.make_async_remote_copy(obuf.at[lax.rem(h, 2)], far_hbm.at[h], o_s.at[h], o_r.at[h], device_id={"sp": opposite},
                                            device_id_type=MESH)

    def l_copy(h):
        return pltpu.make_async_remote_copy(lbuf.at[lax.rem(h, 2)], flse.at[h], l_s.at[h], l_r.at[h], device_id={"sp": opposite},
                                            device_id_type=MESH)

    def kv_load(h):
        return pltpu.make_async_copy(kv_hbm.at[h], kvs.at[h], kv_sem.at[h])

    def load(src, h, slot):
        return pltpu.make_async_copy(src.at[h], qbuf.at[slot], load_sem.at[slot])

    def out_copy(h):
        return pltpu.make_async_copy(obuf.at[lax.rem(h, 2)], seen_hbm.at[h], out_sem.at[lax.rem(h, 2)])

    def each(f):
        lax.fori_loop(0, heads, lambda h, _: f(h), None)

    load(q_hbm, 0, 0).start()
    for h in range(heads):
        kv_load(h).start()

    @pl.when(me < 3)
    def _():
        each(lambda h: near_copy(h).start())

    @pl.when(is_high)
    def _():
        each(lambda h: q_copy(h).start())

    ones = jnp.ones((8, bk), low)

    def block(kv, rows, slot, q, strips, masked, first):
        k = kvs[kv, 0, rows, :]
        scores = [_dot(k, qbuf[q, n, at : at + wide, :], 1, 1) for n, at in strips]
        weights, keeps = [], []
        for (n, at), s, mask in zip(strips, scores, masked):
            c = slice(n * tokens + at, n * tokens + at + wide)
            if mask:
                ok = lax.broadcasted_iota(jnp.int32, (bk, wide), 1) >= lax.broadcasted_iota(jnp.int32, (bk, wide), 0)
                s = jnp.where(ok, s, HIDDEN)
            peak = s.max(axis=0, keepdims=True)
            if not first:
                old = top[slot, :, c]
                peak = jnp.maximum(old, peak)
                keeps.append(jnp.exp2((old - peak) * e))
            top[slot, :, c] = peak
            weights.append(jnp.exp2((s - peak) * e).astype(low))
        values = jnp.concatenate([kvs[kv, 1, rows, :].T, ones], axis=0)
        for i, ((n, at), p) in enumerate(zip(strips, weights)):
            c = slice(n * tokens + at, n * tokens + at + wide)
            new = _dot(values, p, 1, 0)
            mix[slot, :, c] = new if first else mix[slot, :, c] * keeps[i] + new

    everything = [(n, at) for n in range(g) for at in range(0, tokens, wide)]

    def whole(kv, slot, q):
        lax.fori_loop(0, tokens // bk, lambda j, _: block(kv, pl.ds(j * bk, bk), slot, q, everything, [False] * len(everything), False), None)

    def fresh(slot):
        top[slot] = jnp.full((1, cols), NEG, jnp.float32)
        mix[slot] = jnp.zeros((d + 8, cols), jnp.float32)

    def own(h):
        slot = lax.rem(h, 2)
        load(q_hbm, h, slot).wait()
        kv_load(h).wait()

        @pl.when(h + 1 < heads)
        def _():
            load(q_hbm, h + 1, 1 - slot).start()

        for j in range(0, tokens, bk):
            strips = [(n, at) for n, at in everything if at >= j]
            block(h, pl.ds(j, bk), h, slot, strips, [at == j for _, at in strips], j == 0)

    each(own)

    def give(slot, out, far, lse_out=None, lse_far=None):
        for n, at in everything:
            c = slice(n * tokens + at, n * tokens + at + wide)
            total = mix[slot, d : d + 1, c]
            part = 1 / total
            lse = top[slot, :, c] * scale + jnp.log(total)
            if lse_out is not None:
                lbuf[lse_out, :, c] = lse
            if lse_far is not None:
                high = jnp.maximum(lse, flse[lse_far, :, c])
                a, b = jnp.exp(lse - high), jnp.exp(flse[lse_far, :, c] - high)
                part = part * a / (a + b)
                t = mix[slot, :d, c] * part + qbuf[far, n, at : at + wide, :].astype(jnp.float32).T * (b / (a + b))
            else:
                t = mix[slot, :d, c] * part
            obuf[out, n, at : at + wide, :] = t.T.astype(low)

    def visits(h):
        @pl.when(odd)
        def _():
            load(q_hbm, h, 1).start()

        @pl.when(me != 2)
        def _():
            near_copy(h).wait_recv()

        @pl.when(is_low)
        def _():
            q_copy(h).wait_recv()
            load(guest_hbm, h, 0).start()
            fresh(heads)
            load(guest_hbm, h, 0).wait()
            whole(h, heads, 0)
            whole(heads + h, heads, 0)

            @pl.when(h >= 2)
            def _():
                o_copy(h - 2).wait_send()
                l_copy(h - 2).wait_send()

            give(heads, lax.rem(h, 2), None, lse_out=lax.rem(h, 2))
            o_copy(h).start()
            l_copy(h).start()

        @pl.when(odd)
        def _():
            load(q_hbm, h, 1).wait()
            whole(heads + h, h, 1)

    each(visits)

    @pl.when(is_low)
    def _():
        for h in range(heads - 2, heads):
            o_copy(h).wait_send()
            l_copy(h).wait_send()

    def finals(h):
        @pl.when(h >= 2)
        def _():
            out_copy(h - 2).wait()

        @pl.when(is_low)
        def _():
            give(h, lax.rem(h, 2), None)

        @pl.when(is_high)
        def _():
            o_copy(h).wait_recv()
            l_copy(h).wait_recv()
            load(far_hbm, h, 0).start()
            load(far_hbm, h, 0).wait()
            give(h, lax.rem(h, 2), 0, lse_far=h)

        out_copy(h).start()

    each(finals)
    for h in range(heads - 2, heads):
        out_copy(h).wait()

    @pl.when(me < 3)
    def _():
        each(lambda h: near_copy(h).wait_send())

    @pl.when(is_high)
    def _():
        each(lambda h: q_copy(h).wait_send())


def group_attention(q, kv, bk=512):
    heads, g, tokens, d = q.shape
    dma = lambda n: pltpu.SemaphoreType.DMA((n,))
    anywhere = pl.BlockSpec(memory_space=pl.ANY)
    like = jax.ShapeDtypeStruct(q.shape, q.dtype)
    return pl.pallas_call(
        functools.partial(_group, scale=d**-0.5, bk=bk),
        in_specs=[anywhere] * 2,
        out_specs=[anywhere] * 3,
        out_shape=[like] * 3,
        scratch_shapes=[
            pltpu.VMEM((2 * heads, 2, tokens, d), q.dtype),
            pltpu.VMEM((2, g, tokens, d), q.dtype),
            pltpu.VMEM((heads + 1, d + 8, g * tokens), jnp.float32),
            pltpu.VMEM((heads + 1, 1, g * tokens), jnp.float32),
            pltpu.VMEM((2, g, tokens, d), q.dtype),
            pltpu.VMEM((2, 1, g * tokens), jnp.float32),
            pltpu.VMEM((heads, 1, g * tokens), jnp.float32),
            dma(heads), dma(2), dma(heads), dma(heads), dma(heads), dma(heads), dma(heads), dma(heads), dma(heads), dma(heads), dma(2),
        ],
        compiler_params=pltpu.CompilerParams(collective_id=1, has_side_effects=True, vmem_limit_bytes=67043328),
        cost_estimate=pl.CostEstimate(flops=10 * heads * g * tokens * tokens * d, transcendentals=0, bytes_accessed=12 * heads * g * tokens * d),
    )(q, kv)[0]


def _finish(off_ref, x_ref, seen_ref, *rest, pieces):
    w_refs, (y_ref, wbuf, seen_s, sems) = rest[:pieces], rest[pieces:]

    @pl.when(pl.program_id(0) == 0)
    def _():
        _assemble(off_ref, w_refs, wbuf, sems)

    at = 0
    for i in range(seen_ref.shape[0]):
        for n in range(seen_ref.shape[1]):
            seen_s[:, at : at + HEAD] = seen_ref[i, n]
            at += HEAD
    step = 512
    for c in range(0, y_ref.shape[1], step):
        y = _dot(seen_s[...], wbuf[:, c : c + step], 1, 0)
        y_ref[:, c : c + step] = (x_ref[:, c : c + step].astype(jnp.float32) + y).astype(jnp.bfloat16)


def finish(x, seen, offsets, pieces, bm=256):
    tokens, d = x.shape
    k = seen.shape[0] * seen.shape[1] * HEAD
    row = lambda i, _: (i, 0)
    return pl.pallas_call(
        functools.partial(_finish, pieces=len(pieces)),
        grid_spec=pltpu.PrefetchScalarGridSpec(
            num_scalar_prefetch=1,
            grid=(tokens // bm,),
            in_specs=[pl.BlockSpec((bm, d), row), pl.BlockSpec((*seen.shape[:2], bm, HEAD), lambda i, _: (0, 0, i, 0))]
            + [pl.BlockSpec(memory_space=pl.ANY)] * len(pieces),
            out_specs=pl.BlockSpec((bm, d), row),
            scratch_shapes=[pltpu.VMEM((k, d), jnp.bfloat16), pltpu.VMEM((bm, k), jnp.bfloat16), pltpu.SemaphoreType.DMA((len(pieces),))],
        ),
        out_shape=jax.ShapeDtypeStruct((tokens, d), jnp.bfloat16),
        compiler_params=pltpu.CompilerParams(dimension_semantics=("arbitrary",), vmem_limit_bytes=VMEM),
        cost_estimate=pl.CostEstimate(flops=2 * tokens * d * k, transcendentals=0, bytes_accessed=2 * (2 * tokens * d + d * k + 2 * tokens * k)),
    )(offsets, x, seen, *pieces)


def after(value, *others):
    return lax.optimization_barrier((value, *others))[0]


def solution(mesh):
    groups, size = mesh.shape["dp"], mesh.shape["sp"]

    def along(t, way):
        return lax.ppermute(t, ("dp", "sp"), [(g * size + s, g * size + (s + way(g)) % size) for g in range(groups) for s in range(size)])

    def across(t, bit):
        return lax.ppermute(t, "dp", [(g, g ^ bit) for g in range(groups)])

    def hop(t, pairs):
        return lax.ppermute(t, "sp", pairs)

    ahead, back = (lambda g: 1 - 2 * (g % 2)), (lambda g: 2 * (g % 2) - 1)

    def fetch(w, share):
        group, me = lax.axis_index("dp"), lax.axis_index("sp")
        core, second = group % 2, group // 2 % 2
        rows = w.shape[0] // share
        which = core if share == 2 else 2 * core + second
        mine = lax.dynamic_slice_in_dim(w, which * rows, rows, 0)
        near, other = along(mine, ahead), along(mine, back)
        far = along(near, ahead)
        sign = 1 - 2 * core

        def places(sign, which):
            return [((me + size + by) % size) * w.shape[0] + which * rows for by in (-sign, sign, 2)]

        pieces, place = [near, other, far], places(sign, which)
        if share == 4:
            pieces += [across(t, 2) for t in pieces]
            place += places(sign, 2 * core + 1 - second)
        pieces += [across(t, 1) for t in pieces]
        if share == 4:
            place += places(-sign, 2 * (1 - core) + second) + places(-sign, 2 * (1 - core) + 1 - second)
        else:
            place += places(-sign, 1 - core)
        return [w, *pieces], jnp.stack([me * w.shape[0], *place]).astype(jnp.int32)

    def step(x, gain, wq, wk, wv, wo):
        own = x.shape[0]
        me = lax.axis_index("sp")
        width = wk.shape[1] // HEAD
        gain = gain[None]
        wkv = jnp.concatenate([w[:, n * HEAD : (n + 1) * HEAD] for n in range(width) for w in (wk, wv)], axis=1)
        kv_pieces, kv_place = fetch(wkv, 2)
        q_pieces, q_place = fetch(wq, 4)
        half = HEAD // 2
        angle = (me * own + jnp.arange(own)).astype(jnp.float32)[:, None] * THETA ** (-jnp.arange(half, dtype=jnp.float32) / half)
        cos, sin = jnp.cos(angle), jnp.sin(angle)
        kv = project(x, gain, cos, sin, kv_place, kv_pieces, width, (True, False))
        q = project(x, gain, cos, sin, q_place, q_pieces, width, (True, True))
        o_pieces, o_place = fetch(wo, 4)
        return finish(x, group_attention(q, kv), o_place, o_pieces)

    tokens, whole = P(("dp", "sp"), None), P("sp", None)
    return jax.shard_map(
        step,
        mesh=mesh,
        in_specs=(tokens, P(None), whole, whole, whole, whole),
        out_specs=tokens,
        check_vma=False,
    )
```

```python
import functools

import jax
import jax.numpy as jnp
from jax import lax
from jax.experimental import pallas as pl
from jax.experimental.pallas import tpu as pltpu
from jax.sharding import PartitionSpec as P

NEG = -1e30
HIDDEN = 2 * NEG
LOG2E = 1.4426950408889634
VMEM = 56 * 2**20
HEAD = 256
THETA = 10000
STRIP = 512


def _dot(a, b, ca, cb):
    return lax.dot_general(a, b, (((ca,), (cb,)), ((), ())), preferred_element_type=jnp.float32)


MESH = pl.DeviceIdType.MESH
SHARE_KV, SHARE_Q = 2, 4


def _across(group, bit):
    return group + bit - 2 * bit * (group // bit % 2)


def _weights(x_hbm, gain_ref, cos_ref, sin_ref, wq, wk, wv, wo, kv_hbm, q_hbm, wo_hbm, wbuf, a_s, xbuf, obuf, own_sem, x_sem, out_sem,
             ring_s, ring_r, y_s, y_r, c_s, c_r, wo_s, wo_r, *, bm):
    items, depth, _ = wbuf.shape
    tokens, d = x_hbm.shape
    shard, o_shard = wq.shape[0], wo.shape[0]
    low = jnp.bfloat16
    me, group, size = lax.axis_index("sp"), lax.axis_index("dp"), lax.axis_size("sp")
    core, second = lax.rem(group, 2), lax.rem(group // 2, 2)
    sign = 1 - 2 * core
    ahead, behind, far = lax.rem(me + sign + size, size), lax.rem(me - sign + size, size), lax.rem(me + 2, size)

    barrier = pltpu.get_barrier_semaphore()
    for peer in ({"sp": ahead}, {"sp": behind}, {"dp": _across(group, 1)}, {"dp": _across(group, 2)}):
        pl.semaphore_signal(barrier, inc=1, device_id=peer, device_id_type=MESH)
    pl.semaphore_wait(barrier, 4)

    share = lambda i: SHARE_Q if i % 2 else SHARE_KV
    part2, part4, part4y = core, 2 * core + second, 2 * core + 1 - second

    def at(i, j, part):
        rows = shard // share(i)
        return wbuf.at[i, pl.ds(pl.multiple_of(j * shard + part * rows, 32), rows)]

    def send(ref, ss, rs, peer):
        return pltpu.make_async_remote_copy(ref, ref, ss, rs, device_id=peer, device_id_type=MESH)

    mine = lambda i: part4 if share(i) == 4 else part2
    ring = lambda i, k: send(at(i, behind if k == 2 else me, mine(i)), ring_s.at[i, k], ring_r.at[i, k],
                             {"sp": behind if k == 1 else ahead})
    came = (behind, ahead, far)
    over = lambda i, k: send(at(i, came[k], mine(i)), y_s.at[i // 2, k], y_r.at[i // 2, k], {"dp": _across(group, 2)})
    twin = lambda i, k: send(at(i, came[k % 3], mine(i) if k < 3 else part4y), c_s.at[i, k], c_r.at[i, k], {"dp": _across(group, 1)})

    o_rows = o_shard // SHARE_Q

    def o_at(j):
        return wo_hbm.at[pl.ds(pl.multiple_of(j * o_shard + part4 * o_rows, 32), o_rows)]

    def o_ring(k):
        src = o_at(behind) if k == 2 else wo.at[pl.ds(pl.multiple_of(part4 * o_rows, 32), o_rows)]
        return pltpu.make_async_remote_copy(src, o_at(behind if k == 2 else me), wo_s.at[k], wo_r.at[k],
                                            device_id={"sp": behind if k == 1 else ahead}, device_id_type=MESH)

    def own_loads(i):
        n = i // 2
        rows = pl.ds(pl.multiple_of(me * shard, 32), shard)
        if i % 2:
            return [pltpu.make_async_copy(wq.at[:, pl.ds(n * 2 * HEAD, 2 * HEAD)], wbuf.at[i, rows], own_sem.at[i, 0])]
        return [pltpu.make_async_copy(w.at[:, pl.ds(n * HEAD, HEAD)], wbuf.at[i, rows, pl.ds(k * HEAD, HEAD)], own_sem.at[i, k])
                for k, w in enumerate((wk, wv))]

    def x_load(n, slot):
        return pltpu.make_async_copy(x_hbm.at[pl.ds(pl.multiple_of(n * xbuf.shape[1], 32), xbuf.shape[1])], xbuf.at[slot], x_sem.at[slot])

    def out_copy(i):
        return pltpu.make_async_copy(obuf.at[i % 2], (q_hbm if i % 2 else kv_hbm).at[i // 2], out_sem.at[i % 2])

    def launch(i):
        if i < items:
            for c in own_loads(i):
                c.wait()
            ring(i, 0).start()
            ring(i, 1).start()
        elif i == items:
            o_ring(0).start()
            o_ring(1).start()

    def relay(i):
        if i < items:
            ring(i, 0).wait_recv()
            ring(i, 2).start()
            ring(i, 1).wait_recv()
            for k in (0, 1):
                twin(i, k).start()
                if share(i) == 4:
                    over(i, k).start()
        elif i == items:
            o_ring(0).wait_recv()
            o_ring(2).start()
            o_ring(1).wait_recv()

    def relay_far(i):
        if 0 <= i < items:
            ring(i, 2).wait_recv()
            twin(i, 2).start()
            if share(i) == 4:
                over(i, 2).start()

    def relay_over(i):
        if 0 <= i < items and share(i) == 4:
            for k in range(3):
                over(i, k).wait_recv()
                twin(i, k + 3).start()

    def arrive(i):
        for k in range(6 if share(i) == 4 else 3):
            twin(i, k).wait_recv()

    for i in range(items):
        for c in own_loads(i):
            c.start()
    x_load(0, 0).start()
    for i in range(LEAD):
        launch(i)

    def norm(n, _):
        slot = lax.rem(n, 2)

        @pl.when(n + 1 < tokens // xbuf.shape[1])
        def _():
            x_load(n + 1, 1 - slot).start()

        x_load(n, slot).wait()
        wide = xbuf[slot].astype(jnp.float32)
        scale = lax.rsqrt(jnp.mean(wide * wide, -1, keepdims=True) + 1e-6)
        a_s[pl.ds(pl.multiple_of(n * xbuf.shape[1], 32), xbuf.shape[1]), :] = (wide * scale * gain_ref[...].astype(jnp.float32)).astype(low)

    lax.fori_loop(0, tokens // xbuf.shape[1], norm, None)

    def compute(i):
        if i >= 2:
            out_copy(i - 2).wait()

        def rows(r, _):
            here = pl.ds(pl.multiple_of(r * bm, bm), bm)
            both = _dot(a_s[here, :], wbuf[i], 1, 0)
            half = HEAD // 2
            for n in range(2):
                t = both[:, n * HEAD : (n + 1) * HEAD].astype(low)
                if i % 2 or n == 0:
                    a, b = t[:, :half].astype(jnp.float32), t[:, half:].astype(jnp.float32)
                    cos, sin = cos_ref[here, :], sin_ref[here, :]
                    t = jnp.concatenate([a * cos - b * sin, b * cos + a * sin], -1).astype(low)
                obuf[i % 2, n, here, :] = t

        lax.fori_loop(0, tokens // bm, rows, None)
        out_copy(i).start()

    for i in range(-3, items):
        relay(i + 3)
        launch(i + 3 + LEAD)
        relay_far(i + 2)
        relay_over(i + 1)
        if i >= 0:
            arrive(i)
            compute(i)
    for k in range(3):
        if k == 2:
            o_ring(k).wait_recv()
        o_ring(k).wait_send()
    for i in range(items):
        for k in range(3):
            ring(i, k).wait_send()
        for k in range(6 if share(i) == 4 else 3):
            twin(i, k).wait_send()
        if share(i) == 4:
            for k in range(3):
                over(i, k).wait_send()
    out_copy(items - 2).wait()
    out_copy(items - 1).wait()


LEAD = 2


def projections(x, gain, cos, sin, wq, wk, wv, wo, size, bm=512):
    tokens, d = x.shape
    width = wk.shape[1] // HEAD
    items = 2 * width
    dma = lambda *n: pltpu.SemaphoreType.DMA(n)
    anywhere, vmem = pl.BlockSpec(memory_space=pl.ANY), pl.BlockSpec(memory_space=pltpu.VMEM)
    out = jax.ShapeDtypeStruct((width, 2, tokens, HEAD), jnp.bfloat16)
    return pl.pallas_call(
        functools.partial(_weights, bm=bm),
        in_specs=[anywhere, vmem, vmem, vmem, anywhere, anywhere, anywhere, anywhere],
        out_specs=[anywhere] * 3,
        out_shape=[out, out, jax.ShapeDtypeStruct((wo.shape[0] * size, wo.shape[1]), wo.dtype)],
        scratch_shapes=[
            pltpu.VMEM((items, d, 2 * HEAD), jnp.bfloat16),
            pltpu.VMEM((tokens, d), jnp.bfloat16),
            pltpu.VMEM((2, 256, d), jnp.bfloat16),
            pltpu.VMEM((2, 2, tokens, HEAD), jnp.bfloat16),
            dma(items, 2), dma(2), dma(2), dma(items, 3), dma(items, 3), dma(width, 3), dma(width, 3), dma(items, 6), dma(items, 6), dma(3), dma(3),
        ],
        compiler_params=pltpu.CompilerParams(collective_id=2, has_side_effects=True, vmem_limit_bytes=VMEM),
        cost_estimate=pl.CostEstimate(flops=2 * tokens * d * items * 2 * HEAD, transcendentals=0, bytes_accessed=2 * (tokens * d + d * items * 512)),
    )(x, gain, cos, sin, wq, wk, wv, wo)


def _group(q_hbm, kv_hbm, wo_in, seen_hbm, guest_hbm, far_hbm, wo_hbm, kvs, qbuf, mix, top, obuf, lbuf, flse, kv_sem, load_sem, near_s, near_r, q_s, q_r,
           o_s, o_r, l_s, l_r, out_sem, y_s, y_r, c_s, c_r, *, scale, bk):
    heads, g, tokens, d = q_hbm.shape
    low = q_hbm.dtype
    e = scale * LOG2E
    cols = g * tokens
    wide = STRIP
    me = lax.axis_index("sp")
    size = lax.axis_size("sp")
    is_low, is_high, odd = me < 2, me >= 2, lax.rem(me, 2) == 1
    beside, opposite = me + 1 - 2 * lax.rem(me, 2), 3 - me

    barrier = pltpu.get_barrier_semaphore()
    for by in (1, size - 1):
        pl.semaphore_signal(barrier, inc=1, device_id={"sp": lax.rem(me + by, size)}, device_id_type=MESH)
    group = lax.axis_index("dp")
    for bit in (1, 2):
        pl.semaphore_signal(barrier, inc=1, device_id={"dp": _across(group, bit)}, device_id_type=MESH)
    pl.semaphore_wait(barrier, 4)

    part = 2 * lax.rem(group, 2) + lax.rem(group // 2, 2)
    part_y = part + 1 - 2 * lax.rem(group // 2, 2)
    o_shard = wo_hbm.shape[0] // size

    def o_send(k, part, ss, rs, bit):
        rows = o_shard // SHARE_Q
        ref = wo_hbm.at[pl.ds(pl.multiple_of(lax.rem(me + 1 + k, size) * o_shard + part * rows, 32), rows)]
        return pltpu.make_async_remote_copy(ref, ref, ss, rs, device_id={"dp": _across(group, bit)}, device_id_type=MESH)

    over = lambda k: o_send(k, part, y_s.at[k], y_r.at[k], 2)
    twin = lambda k: o_send(k % 3, part if k < 3 else part_y, c_s.at[k], c_r.at[k], 1)

    def near_copy(h):
        return pltpu.make_async_remote_copy(kv_hbm.at[h], kvs.at[heads + h], near_s.at[h], near_r.at[h], device_id={"sp": beside},
                                            device_id_type=MESH)

    def q_copy(h):
        return pltpu.make_async_remote_copy(q_hbm.at[h], guest_hbm.at[h], q_s.at[h], q_r.at[h], device_id={"sp": opposite},
                                            device_id_type=MESH)

    def o_copy(h):
        return pltpu.make_async_remote_copy(obuf.at[lax.rem(h, 2)], far_hbm.at[h], o_s.at[h], o_r.at[h], device_id={"sp": opposite},
                                            device_id_type=MESH)

    def l_copy(h):
        return pltpu.make_async_remote_copy(lbuf.at[lax.rem(h, 2)], flse.at[h], l_s.at[h], l_r.at[h], device_id={"sp": opposite},
                                            device_id_type=MESH)

    def kv_load(h):
        return pltpu.make_async_copy(kv_hbm.at[h], kvs.at[h], kv_sem.at[h])

    def load(src, h, slot):
        return pltpu.make_async_copy(src.at[h], qbuf.at[slot], load_sem.at[slot])

    def out_copy(h):
        return pltpu.make_async_copy(obuf.at[lax.rem(h, 2)], seen_hbm.at[h], out_sem.at[lax.rem(h, 2)])

    def each(f):
        lax.fori_loop(0, heads, lambda h, _: f(h), None)

    load(q_hbm, 0, 0).start()
    for h in range(heads):
        kv_load(h).start()

    @pl.when(me < 3)
    def _():
        each(lambda h: near_copy(h).start())

    @pl.when(is_high)
    def _():
        each(lambda h: q_copy(h).start())

    for k in range(3):
        over(k).start()
        twin(k).start()

    ones = jnp.ones((8, bk), low)

    def block(kv, rows, slot, q, strips, masked, first):
        k = kvs[kv, 0, rows, :]
        scores = [_dot(k, qbuf[q, n, at : at + wide, :], 1, 1) for n, at in strips]
        weights, keeps = [], []
        for (n, at), s, mask in zip(strips, scores, masked):
            c = slice(n * tokens + at, n * tokens + at + wide)
            if mask:
                ok = lax.broadcasted_iota(jnp.int32, (bk, wide), 1) >= lax.broadcasted_iota(jnp.int32, (bk, wide), 0)
                s = jnp.where(ok, s, HIDDEN)
            peak = s.max(axis=0, keepdims=True)
            if not first:
                old = top[slot, :, c]
                peak = jnp.maximum(old, peak)
                keeps.append(jnp.exp2((old - peak) * e))
            top[slot, :, c] = peak
            weights.append(jnp.exp2((s - peak) * e).astype(low))
        values = jnp.concatenate([kvs[kv, 1, rows, :].T, ones], axis=0)
        for i, ((n, at), p) in enumerate(zip(strips, weights)):
            c = slice(n * tokens + at, n * tokens + at + wide)
            new = _dot(values, p, 1, 0)
            mix[slot, :, c] = new if first else mix[slot, :, c] * keeps[i] + new

    everything = [(n, at) for n in range(g) for at in range(0, tokens, wide)]

    def whole(kv, slot, q):
        lax.fori_loop(0, tokens // bk, lambda j, _: block(kv, pl.ds(j * bk, bk), slot, q, everything, [False] * len(everything), False), None)

    def fresh(slot):
        top[slot] = jnp.full((1, cols), NEG, jnp.float32)
        mix[slot] = jnp.zeros((d + 8, cols), jnp.float32)

    def own(h):
        slot = lax.rem(h, 2)
        load(q_hbm, h, slot).wait()
        kv_load(h).wait()

        @pl.when(h + 1 < heads)
        def _():
            load(q_hbm, h + 1, 1 - slot).start()

        for j in range(0, tokens, bk):
            strips = [(n, at) for n, at in everything if at >= j]
            block(h, pl.ds(j, bk), h, slot, strips, [at == j for _, at in strips], j == 0)

    each(own)

    def give(slot, out, far, lse_out=None, lse_far=None):
        for n, at in everything:
            c = slice(n * tokens + at, n * tokens + at + wide)
            total = mix[slot, d : d + 1, c]
            part = 1 / total
            lse = top[slot, :, c] * scale + jnp.log(total)
            if lse_out is not None:
                lbuf[lse_out, :, c] = lse
            if lse_far is not None:
                high = jnp.maximum(lse, flse[lse_far, :, c])
                a, b = jnp.exp(lse - high), jnp.exp(flse[lse_far, :, c] - high)
                part = part * a / (a + b)
                t = mix[slot, :d, c] * part + qbuf[far, n, at : at + wide, :].astype(jnp.float32).T * (b / (a + b))
            else:
                t = mix[slot, :d, c] * part
            obuf[out, n, at : at + wide, :] = t.T.astype(low)

    def visits(h):
        @pl.when(odd)
        def _():
            load(q_hbm, h, 1).start()

        @pl.when(me != 2)
        def _():
            near_copy(h).wait_recv()

        @pl.when(is_low)
        def _():
            q_copy(h).wait_recv()
            load(guest_hbm, h, 0).start()
            fresh(heads)
            load(guest_hbm, h, 0).wait()
            whole(h, heads, 0)
            whole(heads + h, heads, 0)

            @pl.when(h >= 2)
            def _():
                o_copy(h - 2).wait_send()
                l_copy(h - 2).wait_send()

            give(heads, lax.rem(h, 2), None, lse_out=lax.rem(h, 2))
            o_copy(h).start()
            l_copy(h).start()

        @pl.when(odd)
        def _():
            load(q_hbm, h, 1).wait()
            whole(heads + h, h, 1)

    each(visits)
    for k in range(3):
        over(k).wait_recv()
        twin(k + 3).start()

    @pl.when(is_low)
    def _():
        for h in range(heads - 2, heads):
            o_copy(h).wait_send()
            l_copy(h).wait_send()

    def finals(h):
        @pl.when(h >= 2)
        def _():
            out_copy(h - 2).wait()

        @pl.when(is_low)
        def _():
            give(h, lax.rem(h, 2), None)

        @pl.when(is_high)
        def _():
            o_copy(h).wait_recv()
            l_copy(h).wait_recv()
            load(far_hbm, h, 0).start()
            load(far_hbm, h, 0).wait()
            give(h, lax.rem(h, 2), 0, lse_far=h)

        out_copy(h).start()

    each(finals)
    for k in range(6):
        twin(k).wait_recv()
        twin(k).wait_send()
    for k in range(3):
        over(k).wait_send()
    for h in range(heads - 2, heads):
        out_copy(h).wait()

    @pl.when(me < 3)
    def _():
        each(lambda h: near_copy(h).wait_send())

    @pl.when(is_high)
    def _():
        each(lambda h: q_copy(h).wait_send())


def group_attention(q, kv, wo, bk=512):
    heads, g, tokens, d = q.shape
    dma = lambda n: pltpu.SemaphoreType.DMA((n,))
    anywhere = pl.BlockSpec(memory_space=pl.ANY)
    like = jax.ShapeDtypeStruct(q.shape, q.dtype)
    return pl.pallas_call(
        functools.partial(_group, scale=d**-0.5, bk=bk),
        in_specs=[anywhere] * 3,
        out_specs=[anywhere] * 4,
        out_shape=[like] * 3 + [jax.ShapeDtypeStruct(wo.shape, wo.dtype)],
        input_output_aliases={2: 3},
        scratch_shapes=[
            pltpu.VMEM((2 * heads, 2, tokens, d), q.dtype),
            pltpu.VMEM((2, g, tokens, d), q.dtype),
            pltpu.VMEM((heads + 1, d + 8, g * tokens), jnp.float32),
            pltpu.VMEM((heads + 1, 1, g * tokens), jnp.float32),
            pltpu.VMEM((2, g, tokens, d), q.dtype),
            pltpu.VMEM((2, 1, g * tokens), jnp.float32),
            pltpu.VMEM((heads, 1, g * tokens), jnp.float32),
            dma(heads), dma(2), dma(heads), dma(heads), dma(heads), dma(heads), dma(heads), dma(heads), dma(heads), dma(heads), dma(2), dma(3), dma(3), dma(6), dma(6),
        ],
        compiler_params=pltpu.CompilerParams(collective_id=1, has_side_effects=True, vmem_limit_bytes=67043328),
        cost_estimate=pl.CostEstimate(flops=10 * heads * g * tokens * tokens * d, transcendentals=0, bytes_accessed=12 * heads * g * tokens * d),
    )(q, kv, wo)


def _finish(x_ref, seen_ref, own_ref, wo_ref, y_ref, wbuf, seen_s, sems):
    @pl.when(pl.program_id(0) == 0)
    def _():
        me, shard = lax.axis_index("sp"), own_ref.shape[0]
        size = wo_ref.shape[0] // shard
        copies = []
        for k in range(size):
            rows = pl.ds(pl.multiple_of(lax.rem(me + k, size) * shard, 32), shard)
            copies.append(pltpu.make_async_copy(wo_ref.at[rows] if k else own_ref, wbuf.at[rows], sems.at[k]))
        for c in copies:
            c.start()
        for c in copies:
            c.wait()

    at = 0
    for i in range(seen_ref.shape[0]):
        for n in range(seen_ref.shape[1]):
            seen_s[:, at : at + HEAD] = seen_ref[i, n]
            at += HEAD
    step = 512
    for c in range(0, y_ref.shape[1], step):
        y = _dot(seen_s[...], wbuf[:, c : c + step], 1, 0)
        y_ref[:, c : c + step] = (x_ref[:, c : c + step].astype(jnp.float32) + y).astype(jnp.bfloat16)


def finish(x, seen, own, wo, bm=256):
    tokens, d = x.shape
    k = wo.shape[0]
    row = lambda i: (i, 0)
    anywhere = pl.BlockSpec(memory_space=pl.ANY)
    return pl.pallas_call(
        _finish,
        grid=(tokens // bm,),
        in_specs=[pl.BlockSpec((bm, d), row), pl.BlockSpec((*seen.shape[:2], bm, HEAD), lambda i: (0, 0, i, 0)), anywhere, anywhere],
        out_specs=pl.BlockSpec((bm, d), row),
        scratch_shapes=[pltpu.VMEM((k, d), jnp.bfloat16), pltpu.VMEM((bm, k), jnp.bfloat16), pltpu.SemaphoreType.DMA((k // own.shape[0],))],
        out_shape=jax.ShapeDtypeStruct((tokens, d), jnp.bfloat16),
        compiler_params=pltpu.CompilerParams(dimension_semantics=("arbitrary",), vmem_limit_bytes=VMEM),
        cost_estimate=pl.CostEstimate(flops=2 * tokens * d * k, transcendentals=0, bytes_accessed=2 * (2 * tokens * d + d * k + 2 * tokens * k)),
    )(x, seen, own, wo)


def solution(mesh):
    size = mesh.shape["sp"]

    def step(x, gain, wq, wk, wv, wo):
        own = x.shape[0]
        half = HEAD // 2
        place = lax.axis_index("sp") * own + jnp.arange(own)
        angle = place.astype(jnp.float32)[:, None] * THETA ** (-jnp.arange(half, dtype=jnp.float32) / half)
        kv, q, wo_part = projections(x, gain[None], jnp.cos(angle), jnp.sin(angle), wq, wk, wv, wo, size)
        seen, _, _, wo_whole = group_attention(q, kv, wo_part)
        return finish(x, seen, wo, wo_whole)

    tokens, whole = P(("dp", "sp"), None), P("sp", None)
    return jax.shard_map(
        step,
        mesh=mesh,
        in_specs=(tokens, P(None), whole, whole, whole, whole),
        out_specs=tokens,
        check_vma=False,
    )
```

```python
import functools

import jax
import jax.numpy as jnp
from jax import lax
from jax.experimental import pallas as pl
from jax.experimental.pallas import tpu as pltpu
from jax.sharding import PartitionSpec as P

NEG = -1e30
HIDDEN = 2 * NEG
LOG2E = 1.4426950408889634
VMEM = 56 * 2**20
HEAD = 256
THETA = 10000
STRIP = 512


def _dot(a, b, ca, cb):
    return lax.dot_general(a, b, (((ca,), (cb,)), ((), ())), preferred_element_type=jnp.float32)


MESH = pl.DeviceIdType.MESH
SHARE_KV, SHARE_Q = 2, 4


def _across(group, bit):
    return group + bit - 2 * bit * (group // bit % 2)


def _weights(x_hbm, gain_ref, turn_ref, wq, wk, wv, wo, kv_hbm, q_hbm, wo_hbm, wbuf, a_s, cos_ref, sin_ref, xbuf, obuf, own_sem, x_sem, out_sem,
             ring_s, ring_r, y_s, y_r, c_s, c_r, wo_s, wo_r, *, bm):
    items, depth, _ = wbuf.shape
    tokens, d = x_hbm.shape
    shard, o_shard = wq.shape[0], wo.shape[0]
    low = jnp.bfloat16
    me, group, size = lax.axis_index("sp"), lax.axis_index("dp"), lax.axis_size("sp")
    core, second = lax.rem(group, 2), lax.rem(group // 2, 2)
    sign = 1 - 2 * core
    ahead, behind, far = lax.rem(me + sign + size, size), lax.rem(me - sign + size, size), lax.rem(me + 2, size)

    barrier = pltpu.get_barrier_semaphore()
    for peer in ({"sp": ahead}, {"sp": behind}, {"dp": _across(group, 1)}, {"dp": _across(group, 2)}):
        pl.semaphore_signal(barrier, inc=1, device_id=peer, device_id_type=MESH)
    pl.semaphore_wait(barrier, 4)

    share = lambda i: SHARE_Q if i % 2 else SHARE_KV
    part2, part4, part4y = core, 2 * core + second, 2 * core + 1 - second

    def at(i, j, part):
        rows = shard // share(i)
        return wbuf.at[i, pl.ds(pl.multiple_of(j * shard + part * rows, 32), rows)]

    def send(ref, ss, rs, peer):
        return pltpu.make_async_remote_copy(ref, ref, ss, rs, device_id=peer, device_id_type=MESH)

    mine = lambda i: part4 if share(i) == 4 else part2
    ring = lambda i, k: send(at(i, behind if k == 2 else me, mine(i)), ring_s.at[i, k], ring_r.at[i, k],
                             {"sp": behind if k == 1 else ahead})
    came = (behind, ahead, far)
    over = lambda i, k: send(at(i, came[k], mine(i)), y_s.at[i // 2, k], y_r.at[i // 2, k], {"dp": _across(group, 2)})
    twin = lambda i, k: send(at(i, came[k % 3], mine(i) if k < 3 else part4y), c_s.at[i, k], c_r.at[i, k], {"dp": _across(group, 1)})

    o_rows = o_shard // SHARE_Q

    def o_at(j):
        return wo_hbm.at[pl.ds(pl.multiple_of(j * o_shard + part4 * o_rows, 32), o_rows)]

    def o_ring(k):
        src = o_at(behind) if k == 2 else wo.at[pl.ds(pl.multiple_of(part4 * o_rows, 32), o_rows)]
        return pltpu.make_async_remote_copy(src, o_at(behind if k == 2 else me), wo_s.at[k], wo_r.at[k],
                                            device_id={"sp": behind if k == 1 else ahead}, device_id_type=MESH)

    def own_loads(i):
        n = i // 2
        rows = pl.ds(pl.multiple_of(me * shard, 32), shard)
        if i % 2:
            return [pltpu.make_async_copy(wq.at[:, pl.ds(n * 2 * HEAD, 2 * HEAD)], wbuf.at[i, rows], own_sem.at[i, 0])]
        return [pltpu.make_async_copy(w.at[:, pl.ds(n * HEAD, HEAD)], wbuf.at[i, rows, pl.ds(k * HEAD, HEAD)], own_sem.at[i, k])
                for k, w in enumerate((wk, wv))]

    def x_load(n, slot):
        return pltpu.make_async_copy(x_hbm.at[pl.ds(pl.multiple_of(n * xbuf.shape[1], 32), xbuf.shape[1])], xbuf.at[slot], x_sem.at[slot])

    def out_copy(i):
        return pltpu.make_async_copy(obuf.at[i % 2], (q_hbm if i % 2 else kv_hbm).at[i // 2], out_sem.at[i % 2])

    def launch(i):
        if i < items:
            for c in own_loads(i):
                c.wait()
            ring(i, 0).start()
            ring(i, 1).start()
        elif i == items:
            o_ring(0).start()
            o_ring(1).start()

    def relay(i):
        if i < items:
            ring(i, 0).wait_recv()
            ring(i, 2).start()
            ring(i, 1).wait_recv()
            for k in (0, 1):
                twin(i, k).start()
                if share(i) == 4:
                    over(i, k).start()
        elif i == items:
            o_ring(0).wait_recv()
            o_ring(2).start()
            o_ring(1).wait_recv()

    def relay_far(i):
        if 0 <= i < items:
            ring(i, 2).wait_recv()
            twin(i, 2).start()
            if share(i) == 4:
                over(i, 2).start()

    def relay_over(i):
        if 0 <= i < items and share(i) == 4:
            for k in range(3):
                over(i, k).wait_recv()
                twin(i, k + 3).start()

    def arrive(i):
        for k in range(6 if share(i) == 4 else 3):
            twin(i, k).wait_recv()

    for i in range(items):
        for c in own_loads(i):
            c.start()
    x_load(0, 0).start()
    for i in range(LEAD):
        launch(i)

    groups = tokens // FINE
    fine = pl.ds(groups, FINE)

    def spread(n, _):
        here = pl.ds(pl.multiple_of(n * FINE, FINE), FINE)
        cos, sin = turn_ref[0, pl.ds(n, 1), :], turn_ref[1, pl.ds(n, 1), :]
        cos_ref[here, :] = cos * turn_ref[0, fine, :] - sin * turn_ref[1, fine, :]
        sin_ref[here, :] = sin * turn_ref[0, fine, :] + cos * turn_ref[1, fine, :]

    lax.fori_loop(0, groups, spread, None)

    def norm(n, _):
        slot = lax.rem(n, 2)

        @pl.when(n + 1 < tokens // xbuf.shape[1])
        def _():
            x_load(n + 1, 1 - slot).start()

        x_load(n, slot).wait()
        wide = xbuf[slot].astype(jnp.float32)
        scale = lax.rsqrt(jnp.mean(wide * wide, -1, keepdims=True) + 1e-6)
        a_s[pl.ds(pl.multiple_of(n * xbuf.shape[1], 32), xbuf.shape[1]), :] = (wide * scale * gain_ref[...].astype(jnp.float32)).astype(low)

    lax.fori_loop(0, tokens // xbuf.shape[1], norm, None)

    def compute(i):
        if i >= 2:
            out_copy(i - 2).wait()

        def rows(r, _):
            here = pl.ds(pl.multiple_of(r * bm, bm), bm)
            both = _dot(a_s[here, :], wbuf[i], 1, 0)
            half = HEAD // 2
            for n in range(2):
                t = both[:, n * HEAD : (n + 1) * HEAD].astype(low)
                if i % 2 or n == 0:
                    a, b = t[:, :half].astype(jnp.float32), t[:, half:].astype(jnp.float32)
                    cos, sin = cos_ref[here, :], sin_ref[here, :]
                    t = jnp.concatenate([a * cos - b * sin, b * cos + a * sin], -1).astype(low)
                obuf[i % 2, n, here, :] = t

        lax.fori_loop(0, tokens // bm, rows, None)
        out_copy(i).start()

    for i in range(-3, items):
        relay(i + 3)
        launch(i + 3 + LEAD)
        relay_far(i + 2)
        relay_over(i + 1)
        if i >= 0:
            arrive(i)
            compute(i)
    for k in range(3):
        if k == 2:
            o_ring(k).wait_recv()
        o_ring(k).wait_send()
    for i in range(items):
        for k in range(3):
            ring(i, k).wait_send()
        for k in range(6 if share(i) == 4 else 3):
            twin(i, k).wait_send()
        if share(i) == 4:
            for k in range(3):
                over(i, k).wait_send()
    out_copy(items - 2).wait()
    out_copy(items - 1).wait()


LEAD = 2
FINE = 64


def projections(x, gain, turn, wq, wk, wv, wo, size, bm=512):
    tokens, d = x.shape
    width = wk.shape[1] // HEAD
    items = 2 * width
    dma = lambda *n: pltpu.SemaphoreType.DMA(n)
    anywhere, vmem = pl.BlockSpec(memory_space=pl.ANY), pl.BlockSpec(memory_space=pltpu.VMEM)
    out = jax.ShapeDtypeStruct((width, 2, tokens, HEAD), jnp.bfloat16)
    return pl.pallas_call(
        functools.partial(_weights, bm=bm),
        in_specs=[anywhere, vmem, vmem, anywhere, anywhere, anywhere, anywhere],
        out_specs=[anywhere] * 3,
        out_shape=[out, out, jax.ShapeDtypeStruct((wo.shape[0] * size, wo.shape[1]), wo.dtype)],
        scratch_shapes=[
            pltpu.VMEM((items, d, 2 * HEAD), jnp.bfloat16),
            pltpu.VMEM((tokens, d), jnp.bfloat16),
            pltpu.VMEM((tokens, HEAD // 2), jnp.float32),
            pltpu.VMEM((tokens, HEAD // 2), jnp.float32),
            pltpu.VMEM((2, 256, d), jnp.bfloat16),
            pltpu.VMEM((2, 2, tokens, HEAD), jnp.bfloat16),
            dma(items, 2), dma(2), dma(2), dma(items, 3), dma(items, 3), dma(width, 3), dma(width, 3), dma(items, 6), dma(items, 6), dma(3), dma(3),
        ],
        compiler_params=pltpu.CompilerParams(collective_id=2, has_side_effects=True, vmem_limit_bytes=VMEM),
        cost_estimate=pl.CostEstimate(flops=2 * tokens * d * items * 2 * HEAD, transcendentals=0, bytes_accessed=2 * (tokens * d + d * items * 512)),
    )(x, gain, turn, wq, wk, wv, wo)


def _group(q_hbm, kv_hbm, wo_in, seen_hbm, guest_hbm, far_hbm, wo_hbm, kvs, qbuf, mix, top, obuf, lbuf, flse, kv_sem, load_sem, near_s, near_r, q_s, q_r,
           o_s, o_r, l_s, l_r, out_sem, y_s, y_r, c_s, c_r, zero_s, zero_r, one_s, one_r, *, scale, bk):
    heads, g, tokens, d = q_hbm.shape
    low = q_hbm.dtype
    e = scale * LOG2E
    cols = g * tokens
    wide = STRIP
    me = lax.axis_index("sp")
    size = lax.axis_size("sp")
    is_low, is_high, odd = me < 2, me >= 2, lax.rem(me, 2) == 1
    beside, opposite = me + 1 - 2 * lax.rem(me, 2), 3 - me

    barrier = pltpu.get_barrier_semaphore()
    for by in (1, size - 1):
        pl.semaphore_signal(barrier, inc=1, device_id={"sp": lax.rem(me + by, size)}, device_id_type=MESH)
    group = lax.axis_index("dp")
    for bit in (1, 2):
        pl.semaphore_signal(barrier, inc=1, device_id={"dp": _across(group, bit)}, device_id_type=MESH)
    pl.semaphore_wait(barrier, 4)

    part = 2 * lax.rem(group, 2) + lax.rem(group // 2, 2)
    part_y = part + 1 - 2 * lax.rem(group // 2, 2)
    o_shard = wo_hbm.shape[0] // size

    def o_send(k, part, ss, rs, bit):
        rows = o_shard // SHARE_Q
        ref = wo_hbm.at[pl.ds(pl.multiple_of(lax.rem(me + 1 + k, size) * o_shard + part * rows, 32), rows)]
        return pltpu.make_async_remote_copy(ref, ref, ss, rs, device_id={"dp": _across(group, bit)}, device_id_type=MESH)

    over = lambda k: o_send(k, part, y_s.at[k], y_r.at[k], 2)
    twin = lambda k: o_send(k % 3, part if k < 3 else part_y, c_s.at[k], c_r.at[k], 1)

    def near_copy(h):
        return pltpu.make_async_remote_copy(kv_hbm.at[h], kvs.at[heads + h], near_s.at[h], near_r.at[h], device_id={"sp": beside},
                                            device_id_type=MESH)

    def q_copy(h):
        return pltpu.make_async_remote_copy(q_hbm.at[h], guest_hbm.at[h], q_s.at[h], q_r.at[h], device_id={"sp": opposite},
                                            device_id_type=MESH)

    def o_copy(h):
        return pltpu.make_async_remote_copy(obuf.at[lax.rem(h, 2)], far_hbm.at[h], o_s.at[h], o_r.at[h], device_id={"sp": opposite},
                                            device_id_type=MESH)

    def l_copy(h):
        return pltpu.make_async_remote_copy(lbuf.at[lax.rem(h, 2)], flse.at[h], l_s.at[h], l_r.at[h], device_id={"sp": opposite},
                                            device_id_type=MESH)

    def kv_load(h):
        return pltpu.make_async_copy(kv_hbm.at[h], kvs.at[h], kv_sem.at[h])

    def load(src, h, slot):
        return pltpu.make_async_copy(src.at[h], qbuf.at[slot], load_sem.at[slot])

    def out_copy(h):
        return pltpu.make_async_copy(obuf.at[lax.rem(h, 2)], seen_hbm.at[h], out_sem.at[lax.rem(h, 2)])

    def each(f, first=0, last=heads):
        lax.fori_loop(first, last, lambda h, _: f(h), None)

    carried = heads - 1
    zero, one = 2 * heads, 2 * heads + 1
    zero_first = pltpu.make_async_remote_copy(kv_hbm.at[carried], kvs.at[zero], zero_s, zero_r, device_id={"sp": opposite}, device_id_type=MESH)
    zero_next = pltpu.make_async_remote_copy(kvs.at[zero], kvs.at[zero], zero_s, zero_r, device_id={"sp": beside}, device_id_type=MESH)
    one_first = pltpu.make_async_remote_copy(kv_hbm.at[carried], kvs.at[one], one_s.at[2], one_r.at[2], device_id={"sp": opposite},
                                             device_id_type=MESH)

    def one_next(k):
        ref = kvs.at[one, :, pl.ds(k * (tokens // 2), tokens // 2)]
        return pltpu.make_async_remote_copy(ref, ref, one_s.at[k], one_r.at[k], device_id={"sp": beside}, device_id_type=MESH)

    load(q_hbm, 0, 0).start()
    for h in range(heads):
        kv_load(h).start()

    nears = heads - (me == 1).astype(jnp.int32)

    @pl.when(me < 3)
    def _():
        each(lambda h: near_copy(h).start(), 0, nears)

    @pl.when(is_high)
    def _():
        each(lambda h: q_copy(h).start(), 0, carried)

    @pl.when(me == 0)
    def _():
        zero_first.start()

    @pl.when(me == 1)
    def _():
        one_first.start()

    for k in range(3):
        over(k).start()
        twin(k).start()

    ones = jnp.ones((8, bk), low)

    def block(kv, rows, slot, q, strips, masked, first):
        k = kvs[kv, 0, rows, :]
        scores = [_dot(k, qbuf[q, n, at : at + wide, :], 1, 1) for n, at in strips]
        weights, keeps = [], []
        for (n, at), s, mask in zip(strips, scores, masked):
            c = slice(n * tokens + at, n * tokens + at + wide)
            if mask:
                ok = lax.broadcasted_iota(jnp.int32, (bk, wide), 1) >= lax.broadcasted_iota(jnp.int32, (bk, wide), 0)
                s = jnp.where(ok, s, HIDDEN)
            peak = s.max(axis=0, keepdims=True)
            if not first:
                old = top[slot, :, c]
                peak = jnp.maximum(old, peak)
                keeps.append(jnp.exp2((old - peak) * e))
            top[slot, :, c] = peak
            weights.append(jnp.exp2((s - peak) * e).astype(low))
        values = jnp.concatenate([kvs[kv, 1, rows, :].T, ones], axis=0)
        for i, ((n, at), p) in enumerate(zip(strips, weights)):
            c = slice(n * tokens + at, n * tokens + at + wide)
            new = _dot(values, p, 1, 0)
            mix[slot, :, c] = new if first else mix[slot, :, c] * keeps[i] + new

    everything = [(n, at) for n in range(g) for at in range(0, tokens, wide)]

    per = tokens // bk

    def whole(kv, slot, q, first=0, last=per, more=None):
        def step(j, _):
            at = kv if more is None else jnp.where(j < per, kv, more)
            block(at, pl.ds(pl.multiple_of(lax.rem(j, per) * bk, bk), bk), slot, q, everything, [False] * len(everything), False)

        lax.fori_loop(first, last, step, None)

    def fresh(slot):
        top[slot] = jnp.full((1, cols), NEG, jnp.float32)
        mix[slot] = jnp.zeros((d + 8, cols), jnp.float32)

    def own(h):
        slot = lax.rem(h, 2)
        load(q_hbm, h, slot).wait()
        kv_load(h).wait()

        @pl.when(h + 1 < heads)
        def _():
            load(q_hbm, h + 1, 1 - slot).start()

        for j in range(0, tokens, bk):
            strips = [(n, at) for n, at in everything if at >= j]
            block(h, pl.ds(j, bk), h, slot, strips, [at == j for _, at in strips], j == 0)

    each(own)

    def give(slot, out, far, lse_out=None, lse_far=None):
        for n, at in everything:
            c = slice(n * tokens + at, n * tokens + at + wide)
            total = mix[slot, d : d + 1, c]
            part = 1 / total
            lse = top[slot, :, c] * scale + jnp.log(total)
            if lse_out is not None:
                lbuf[lse_out, :, c] = lse
            if lse_far is not None:
                high = jnp.maximum(lse, flse[lse_far, :, c])
                a, b = jnp.exp(lse - high), jnp.exp(flse[lse_far, :, c] - high)
                part = part * a / (a + b)
                t = mix[slot, :d, c] * part + qbuf[far, n, at : at + wide, :].astype(jnp.float32).T * (b / (a + b))
            else:
                t = mix[slot, :d, c] * part
            obuf[out, n, at : at + wide, :] = t.T.astype(low)

    @pl.when(is_high)
    def _():
        load(q_hbm, carried, 1).start()

        @pl.when(me == 2)
        def _():
            one_first.wait_recv()
            one_next(0).start()
            one_next(1).start()

        @pl.when(me == 3)
        def _():
            zero_first.wait_recv()
            zero_next.start()

        load(q_hbm, carried, 1).wait()
        whole(zero + 3 - me, carried, 1)

    def visits(h):
        @pl.when(odd)
        def _():
            load(q_hbm, h, 1).start()

        @pl.when(odd | ((me == 0) & (h < carried)))
        def _():
            near_copy(h).wait_recv()

        @pl.when(is_low & (h < carried))
        def _():
            q_copy(h).wait_recv()
            load(guest_hbm, h, 0).start()
            fresh(heads)
            load(guest_hbm, h, 0).wait()
            whole(h, heads, 0, 0, 2 * per, heads + h)

            @pl.when(h >= 2)
            def _():
                o_copy(h - 2).wait_send()
                l_copy(h - 2).wait_send()

            give(heads, lax.rem(h, 2), None, lse_out=lax.rem(h, 2))
            o_copy(h).start()
            l_copy(h).start()

        @pl.when(odd)
        def _():
            load(q_hbm, h, 1).wait()
            whole(heads + h, h, 1)

    each(visits)
    for k in range(3):
        over(k).wait_recv()
        twin(k + 3).start()

    @pl.when(is_low)
    def _():
        for h in range(carried - 2, carried):
            o_copy(h).wait_send()
            l_copy(h).wait_send()

    def rest():
        load(q_hbm, carried, 1).start()
        load(q_hbm, carried, 1).wait()

        def half(k, _):
            @pl.when((me == 2) & (k == 0))
            def _():
                zero_next.wait_recv()

            @pl.when(me == 3)
            def _():
                one_next(k).wait_recv()

            whole(zero + me - 2, carried, 1, k * (per // 2), (k + 1) * (per // 2))

        lax.fori_loop(0, 2, half, None)

    def finals(h):
        @pl.when(is_high & (h == carried))
        def _():
            rest()

        @pl.when(h >= 2)
        def _():
            out_copy(h - 2).wait()

        @pl.when(is_low | (h == carried))
        def _():
            give(h, lax.rem(h, 2), None)

        @pl.when(is_high & (h < carried))
        def _():
            o_copy(h).wait_recv()
            l_copy(h).wait_recv()
            load(far_hbm, h, 0).start()
            load(far_hbm, h, 0).wait()
            give(h, lax.rem(h, 2), 0, lse_far=h)

        out_copy(h).start()

    each(finals)
    for k in range(6):
        twin(k).wait_recv()
        twin(k).wait_send()
    for k in range(3):
        over(k).wait_send()
    for h in range(heads - 2, heads):
        out_copy(h).wait()

    @pl.when(me < 3)
    def _():
        each(lambda h: near_copy(h).wait_send(), 0, nears)

    @pl.when(is_high)
    def _():
        each(lambda h: q_copy(h).wait_send(), 0, carried)

    @pl.when(me == 0)
    def _():
        zero_first.wait_send()

    @pl.when(me == 1)
    def _():
        one_first.wait_send()

    @pl.when(me == 2)
    def _():
        one_next(0).wait_send()
        one_next(1).wait_send()

    @pl.when(me == 3)
    def _():
        zero_next.wait_send()


def group_attention(q, kv, wo, bk=512):
    heads, g, tokens, d = q.shape
    dma = lambda n: pltpu.SemaphoreType.DMA((n,))
    anywhere = pl.BlockSpec(memory_space=pl.ANY)
    like = jax.ShapeDtypeStruct(q.shape, q.dtype)
    return pl.pallas_call(
        functools.partial(_group, scale=d**-0.5, bk=bk),
        in_specs=[anywhere] * 3,
        out_specs=[anywhere] * 4,
        out_shape=[like] * 3 + [jax.ShapeDtypeStruct(wo.shape, wo.dtype)],
        input_output_aliases={2: 3},
        scratch_shapes=[
            pltpu.VMEM((2 * heads + 2, 2, tokens, d), q.dtype),
            pltpu.VMEM((2, g, tokens, d), q.dtype),
            pltpu.VMEM((heads + 1, d + 8, g * tokens), jnp.float32),
            pltpu.VMEM((heads + 1, 1, g * tokens), jnp.float32),
            pltpu.VMEM((2, g, tokens, d), q.dtype),
            pltpu.VMEM((2, 1, g * tokens), jnp.float32),
            pltpu.VMEM((heads, 1, g * tokens), jnp.float32),
            dma(heads), dma(2), dma(heads), dma(heads), dma(heads), dma(heads), dma(heads), dma(heads), dma(heads), dma(heads), dma(2), dma(3), dma(3), dma(6), dma(6),
            pltpu.SemaphoreType.DMA, pltpu.SemaphoreType.DMA, dma(3), dma(3),
        ],
        compiler_params=pltpu.CompilerParams(collective_id=1, has_side_effects=True, vmem_limit_bytes=67043328),
        cost_estimate=pl.CostEstimate(flops=10 * heads * g * tokens * tokens * d, transcendentals=0, bytes_accessed=12 * heads * g * tokens * d),
    )(q, kv, wo)


def _finish(x_ref, seen_ref, own_ref, wo_ref, y_ref, wbuf, seen_s, sems):
    @pl.when(pl.program_id(0) == 0)
    def _():
        me, shard = lax.axis_index("sp"), own_ref.shape[0]
        size = wo_ref.shape[0] // shard
        copies = []
        for k in range(size):
            rows = pl.ds(pl.multiple_of(lax.rem(me + k, size) * shard, 32), shard)
            copies.append(pltpu.make_async_copy(wo_ref.at[rows] if k else own_ref, wbuf.at[rows], sems.at[k]))
        for c in copies:
            c.start()
        for c in copies:
            c.wait()

    at = 0
    for i in range(seen_ref.shape[0]):
        for n in range(seen_ref.shape[1]):
            seen_s[:, at : at + HEAD] = seen_ref[i, n]
            at += HEAD
    step = 512
    for c in range(0, y_ref.shape[1], step):
        y = _dot(seen_s[...], wbuf[:, c : c + step], 1, 0)
        y_ref[:, c : c + step] = (x_ref[:, c : c + step].astype(jnp.float32) + y).astype(jnp.bfloat16)


def finish(x, seen, own, wo, bm=256):
    tokens, d = x.shape
    k = wo.shape[0]
    row = lambda i: (i, 0)
    anywhere = pl.BlockSpec(memory_space=pl.ANY)
    return pl.pallas_call(
        _finish,
        grid=(tokens // bm,),
        in_specs=[pl.BlockSpec((bm, d), row), pl.BlockSpec((*seen.shape[:2], bm, HEAD), lambda i: (0, 0, i, 0)), anywhere, anywhere],
        out_specs=pl.BlockSpec((bm, d), row),
        scratch_shapes=[pltpu.VMEM((k, d), jnp.bfloat16), pltpu.VMEM((bm, k), jnp.bfloat16), pltpu.SemaphoreType.DMA((k // own.shape[0],))],
        out_shape=jax.ShapeDtypeStruct((tokens, d), jnp.bfloat16),
        compiler_params=pltpu.CompilerParams(dimension_semantics=("arbitrary",), vmem_limit_bytes=VMEM),
        cost_estimate=pl.CostEstimate(flops=2 * tokens * d * k, transcendentals=0, bytes_accessed=2 * (2 * tokens * d + d * k + 2 * tokens * k)),
    )(x, seen, own, wo)


def solution(mesh):
    size = mesh.shape["sp"]

    def step(x, gain, wq, wk, wv, wo):
        own = x.shape[0]
        half = HEAD // 2
        place = jnp.concatenate([lax.axis_index("sp") * own + jnp.arange(0, own, FINE), jnp.arange(FINE)])
        angle = place.astype(jnp.float32)[:, None] * THETA ** (-jnp.arange(half, dtype=jnp.float32) / half)
        turn = jnp.stack([jnp.cos(angle), jnp.sin(angle)])
        kv, q, wo_part = projections(x, gain[None], turn, wq, wk, wv, wo, size)
        seen, _, _, wo_whole = group_attention(q, kv, wo_part)
        return finish(x, seen, wo, wo_whole)

    tokens, whole = P(("dp", "sp"), None), P("sp", None)
    return jax.shard_map(
        step,
        mesh=mesh,
        in_specs=(tokens, P(None), whole, whole, whole, whole),
        out_specs=tokens,
        check_vma=False,
    )
```

```python
import functools

import jax
import jax.numpy as jnp
from jax import lax
from jax.experimental import pallas as pl
from jax.experimental.pallas import tpu as pltpu
from jax.sharding import PartitionSpec as P

NEG = -1e30
HIDDEN = 2 * NEG
LOG2E = 1.4426950408889634
VMEM = 56 * 2**20
HEAD = 256
THETA = 10000
STRIP = 512


def _dot(a, b, ca, cb):
    return lax.dot_general(a, b, (((ca,), (cb,)), ((), ())), preferred_element_type=jnp.float32)


MESH = pl.DeviceIdType.MESH
SHARE_KV, SHARE_Q = 2, 4


def _across(group, bit):
    return group + bit - 2 * bit * (group // bit % 2)


def _weights(x_hbm, gain_ref, turn_ref, wq, wk, wv, wo, kv_hbm, q_hbm, wo_hbm, wbuf, a_s, cos_ref, sin_ref, xbuf, obuf, own_sem, x_sem, out_sem,
             ring_s, ring_r, y_s, y_r, c_s, c_r, wo_s, wo_r, *, bm):
    items, depth, _ = wbuf.shape
    tokens, d = x_hbm.shape
    shard, o_shard = wq.shape[0], wo.shape[0]
    low = jnp.bfloat16
    me, group, size = lax.axis_index("sp"), lax.axis_index("dp"), lax.axis_size("sp")
    core, second = lax.rem(group, 2), lax.rem(group // 2, 2)
    sign = 1 - 2 * core
    ahead, behind, far = lax.rem(me + sign + size, size), lax.rem(me - sign + size, size), lax.rem(me + 2, size)

    barrier = pltpu.get_barrier_semaphore()
    for peer in ({"sp": ahead}, {"sp": behind}, {"dp": _across(group, 1)}, {"dp": _across(group, 2)}):
        pl.semaphore_signal(barrier, inc=1, device_id=peer, device_id_type=MESH)
    pl.semaphore_wait(barrier, 4)

    share = lambda i: SHARE_Q if i % 2 else SHARE_KV
    part2, part4, part4y = core, 2 * core + second, 2 * core + 1 - second

    def at(i, j, part):
        rows = shard // share(i)
        return wbuf.at[i, pl.ds(pl.multiple_of(j * shard + part * rows, 32), rows)]

    def send(ref, ss, rs, peer):
        return pltpu.make_async_remote_copy(ref, ref, ss, rs, device_id=peer, device_id_type=MESH)

    mine = lambda i: part4 if share(i) == 4 else part2
    ring = lambda i, k: send(at(i, behind if k == 2 else me, mine(i)), ring_s.at[i, k], ring_r.at[i, k],
                             {"sp": behind if k == 1 else ahead})
    came = (behind, ahead, far)
    over = lambda i, k: send(at(i, came[k], mine(i)), y_s.at[i // 2, k], y_r.at[i // 2, k], {"dp": _across(group, 2)})
    twin = lambda i, k: send(at(i, came[k % 3], mine(i) if k < 3 else part4y), c_s.at[i, k], c_r.at[i, k], {"dp": _across(group, 1)})

    o_rows = o_shard // SHARE_Q

    def o_at(j):
        return wo_hbm.at[pl.ds(pl.multiple_of(j * o_shard + part4 * o_rows, 32), o_rows)]

    def o_ring(k):
        src = o_at(behind) if k == 2 else wo.at[pl.ds(pl.multiple_of(part4 * o_rows, 32), o_rows)]
        return pltpu.make_async_remote_copy(src, o_at(behind if k == 2 else me), wo_s.at[k], wo_r.at[k],
                                            device_id={"sp": behind if k == 1 else ahead}, device_id_type=MESH)

    def own_loads(i):
        n = i // 2
        rows = pl.ds(pl.multiple_of(me * shard, 32), shard)
        if i % 2:
            return [pltpu.make_async_copy(wq.at[:, pl.ds(n * 2 * HEAD, 2 * HEAD)], wbuf.at[i, rows], own_sem.at[i, 0])]
        return [pltpu.make_async_copy(w.at[:, pl.ds(n * HEAD, HEAD)], wbuf.at[i, rows, pl.ds(k * HEAD, HEAD)], own_sem.at[i, k])
                for k, w in enumerate((wk, wv))]

    def x_load(n, slot):
        return pltpu.make_async_copy(x_hbm.at[pl.ds(pl.multiple_of(n * xbuf.shape[1], 32), xbuf.shape[1])], xbuf.at[slot], x_sem.at[slot])

    def out_copy(i):
        return pltpu.make_async_copy(obuf.at[i % 2], (q_hbm if i % 2 else kv_hbm).at[i // 2], out_sem.at[i % 2])

    def launch(i):
        if i < items:
            for c in own_loads(i):
                c.wait()
            ring(i, 0).start()
            ring(i, 1).start()
        elif i == items:
            o_ring(0).start()
            o_ring(1).start()

    def relay(i):
        if i < items:
            ring(i, 0).wait_recv()
            ring(i, 2).start()
            ring(i, 1).wait_recv()
            for k in (0, 1):
                twin(i, k).start()
                if share(i) == 4:
                    over(i, k).start()
        elif i == items:
            o_ring(0).wait_recv()
            o_ring(2).start()
            o_ring(1).wait_recv()

    def relay_far(i):
        if 0 <= i < items:
            ring(i, 2).wait_recv()
            twin(i, 2).start()
            if share(i) == 4:
                over(i, 2).start()

    def relay_over(i):
        if 0 <= i < items and share(i) == 4:
            for k in range(3):
                over(i, k).wait_recv()
                twin(i, k + 3).start()

    def arrive(i):
        for k in range(6 if share(i) == 4 else 3):
            twin(i, k).wait_recv()

    for i in range(items):
        for c in own_loads(i):
            c.start()
    x_load(0, 0).start()
    for i in range(LEAD):
        launch(i)

    groups = tokens // FINE
    fine = pl.ds(groups, FINE)

    def spread(n, _):
        here = pl.ds(pl.multiple_of(n * FINE, FINE), FINE)
        cos, sin = turn_ref[0, pl.ds(n, 1), :], turn_ref[1, pl.ds(n, 1), :]
        cos_ref[here, :] = cos * turn_ref[0, fine, :] - sin * turn_ref[1, fine, :]
        sin_ref[here, :] = sin * turn_ref[0, fine, :] + cos * turn_ref[1, fine, :]

    lax.fori_loop(0, groups, spread, None)

    def norm(n, _):
        slot = lax.rem(n, 2)

        @pl.when(n + 1 < tokens // xbuf.shape[1])
        def _():
            x_load(n + 1, 1 - slot).start()

        x_load(n, slot).wait()
        wide = xbuf[slot].astype(jnp.float32)
        scale = lax.rsqrt(jnp.mean(wide * wide, -1, keepdims=True) + 1e-6)
        a_s[pl.ds(pl.multiple_of(n * xbuf.shape[1], 32), xbuf.shape[1]), :] = (wide * scale * gain_ref[...].astype(jnp.float32)).astype(low)

    lax.fori_loop(0, tokens // xbuf.shape[1], norm, None)

    def compute(i):
        if i >= 2:
            out_copy(i - 2).wait()

        def rows(r, _):
            here = pl.ds(pl.multiple_of(r * bm, bm), bm)
            both = _dot(a_s[here, :], wbuf[i], 1, 0)
            half = HEAD // 2
            for n in range(2):
                t = both[:, n * HEAD : (n + 1) * HEAD].astype(low)
                if i % 2 or n == 0:
                    a, b = t[:, :half].astype(jnp.float32), t[:, half:].astype(jnp.float32)
                    cos, sin = cos_ref[here, :], sin_ref[here, :]
                    t = jnp.concatenate([a * cos - b * sin, b * cos + a * sin], -1).astype(low)
                obuf[i % 2, n, here, :] = t

        lax.fori_loop(0, tokens // bm, rows, None)
        out_copy(i).start()

    for i in range(2):
        relay(i)
        launch(i + LEAD)
    relay_far(0)
    for i in range(items):
        arrive(i)
        if i == items - 1:
            relay(items)
        compute(i)
        if i == 0:
            relay(2)
            launch(2 + LEAD)
            relay_far(1)
        if i + 3 < items:
            relay(i + 3)
        launch(i + 3 + LEAD)
        relay_far(i + 2)
        relay_over(i + 1)
    for k in range(3):
        if k == 2:
            o_ring(k).wait_recv()
        o_ring(k).wait_send()
    for i in range(items):
        for k in range(3):
            ring(i, k).wait_send()
        for k in range(6 if share(i) == 4 else 3):
            twin(i, k).wait_send()
        if share(i) == 4:
            for k in range(3):
                over(i, k).wait_send()
    out_copy(items - 2).wait()
    out_copy(items - 1).wait()


LEAD = 2
FINE = 64


def projections(x, gain, turn, wq, wk, wv, wo, size, bm=512):
    tokens, d = x.shape
    width = wk.shape[1] // HEAD
    items = 2 * width
    dma = lambda *n: pltpu.SemaphoreType.DMA(n)
    anywhere, vmem = pl.BlockSpec(memory_space=pl.ANY), pl.BlockSpec(memory_space=pltpu.VMEM)
    out = jax.ShapeDtypeStruct((width, 2, tokens, HEAD), jnp.bfloat16)
    return pl.pallas_call(
        functools.partial(_weights, bm=bm),
        in_specs=[anywhere, vmem, vmem, anywhere, anywhere, anywhere, anywhere],
        out_specs=[anywhere] * 3,
        out_shape=[out, out, jax.ShapeDtypeStruct((wo.shape[0] * size, wo.shape[1]), wo.dtype)],
        scratch_shapes=[
            pltpu.VMEM((items, d, 2 * HEAD), jnp.bfloat16),
            pltpu.VMEM((tokens, d), jnp.bfloat16),
            pltpu.VMEM((tokens, HEAD // 2), jnp.float32),
            pltpu.VMEM((tokens, HEAD // 2), jnp.float32),
            pltpu.VMEM((2, 256, d), jnp.bfloat16),
            pltpu.VMEM((2, 2, tokens, HEAD), jnp.bfloat16),
            dma(items, 2), dma(2), dma(2), dma(items, 3), dma(items, 3), dma(width, 3), dma(width, 3), dma(items, 6), dma(items, 6), dma(3), dma(3),
        ],
        compiler_params=pltpu.CompilerParams(collective_id=2, has_side_effects=True, vmem_limit_bytes=VMEM),
        cost_estimate=pl.CostEstimate(flops=2 * tokens * d * items * 2 * HEAD, transcendentals=0, bytes_accessed=2 * (tokens * d + d * items * 512)),
    )(x, gain, turn, wq, wk, wv, wo)


def _group(q_hbm, kv_hbm, wo_in, seen_hbm, guest_hbm, far_hbm, wo_hbm, kvs, qbuf, mix, top, obuf, lbuf, flse, kv_sem, load_sem, near_s, near_r, q_s, q_r,
           o_s, o_r, l_s, l_r, out_sem, y_s, y_r, c_s, c_r, zero_s, zero_r, one_s, one_r, *, scale, bk):
    heads, g, tokens, d = q_hbm.shape
    low = q_hbm.dtype
    e = scale * LOG2E
    cols = g * tokens
    wide = STRIP
    me = lax.axis_index("sp")
    size = lax.axis_size("sp")
    is_low, is_high, odd = me < 2, me >= 2, lax.rem(me, 2) == 1
    beside, opposite = me + 1 - 2 * lax.rem(me, 2), 3 - me

    barrier = pltpu.get_barrier_semaphore()
    for by in (1, size - 1):
        pl.semaphore_signal(barrier, inc=1, device_id={"sp": lax.rem(me + by, size)}, device_id_type=MESH)
    group = lax.axis_index("dp")
    for bit in (1, 2):
        pl.semaphore_signal(barrier, inc=1, device_id={"dp": _across(group, bit)}, device_id_type=MESH)
    pl.semaphore_wait(barrier, 4)

    part = 2 * lax.rem(group, 2) + lax.rem(group // 2, 2)
    part_y = part + 1 - 2 * lax.rem(group // 2, 2)
    o_shard = wo_hbm.shape[0] // size

    def o_send(k, part, ss, rs, bit):
        rows = o_shard // SHARE_Q
        ref = wo_hbm.at[pl.ds(pl.multiple_of(lax.rem(me + 1 + k, size) * o_shard + part * rows, 32), rows)]
        return pltpu.make_async_remote_copy(ref, ref, ss, rs, device_id={"dp": _across(group, bit)}, device_id_type=MESH)

    over = lambda k: o_send(k, part, y_s.at[k], y_r.at[k], 2)
    twin = lambda k: o_send(k % 3, part if k < 3 else part_y, c_s.at[k], c_r.at[k], 1)

    def near_copy(h):
        return pltpu.make_async_remote_copy(kv_hbm.at[h], kvs.at[heads + h], near_s.at[h], near_r.at[h], device_id={"sp": beside},
                                            device_id_type=MESH)

    def q_copy(h):
        return pltpu.make_async_remote_copy(q_hbm.at[h], guest_hbm.at[h], q_s.at[h], q_r.at[h], device_id={"sp": opposite},
                                            device_id_type=MESH)

    def o_copy(h):
        return pltpu.make_async_remote_copy(obuf.at[lax.rem(h, 2)], far_hbm.at[h], o_s.at[h], o_r.at[h], device_id={"sp": opposite},
                                            device_id_type=MESH)

    def l_copy(h):
        return pltpu.make_async_remote_copy(lbuf.at[lax.rem(h, 2)], flse.at[h], l_s.at[h], l_r.at[h], device_id={"sp": opposite},
                                            device_id_type=MESH)

    def kv_load(h):
        return pltpu.make_async_copy(kv_hbm.at[h], kvs.at[h], kv_sem.at[h])

    def load(src, h, slot):
        return pltpu.make_async_copy(src.at[h], qbuf.at[slot], load_sem.at[slot])

    def out_copy(h):
        return pltpu.make_async_copy(obuf.at[lax.rem(h, 2)], seen_hbm.at[h], out_sem.at[lax.rem(h, 2)])

    def each(f, first=0, last=heads):
        lax.fori_loop(first, last, lambda h, _: f(h), None)

    carried = heads - 1
    zero, one = 2 * heads, 2 * heads + 1
    zero_first = pltpu.make_async_remote_copy(kv_hbm.at[carried], kvs.at[zero], zero_s, zero_r, device_id={"sp": opposite}, device_id_type=MESH)
    zero_next = pltpu.make_async_remote_copy(kvs.at[zero], kvs.at[zero], zero_s, zero_r, device_id={"sp": beside}, device_id_type=MESH)
    one_first = pltpu.make_async_remote_copy(kv_hbm.at[carried], kvs.at[one], one_s.at[3], one_r.at[3], device_id={"sp": opposite},
                                             device_id_type=MESH)

    thirds = (0, tokens // 2, tokens * 3 // 4, tokens)

    def one_next(k):
        ref = kvs.at[one, :, pl.ds(thirds[k], thirds[k + 1] - thirds[k])]
        return pltpu.make_async_remote_copy(ref, ref, one_s.at[k], one_r.at[k], device_id={"sp": beside}, device_id_type=MESH)

    load(q_hbm, 0, 0).start()
    for h in range(heads):
        kv_load(h).start()

    nears = heads - (me == 1).astype(jnp.int32)

    @pl.when(me < 3)
    def _():
        each(lambda h: near_copy(h).start(), 0, nears)

    @pl.when(is_high)
    def _():
        each(lambda h: q_copy(h).start(), 0, carried)

    @pl.when(me == 0)
    def _():
        zero_first.start()

    @pl.when(me == 1)
    def _():
        one_first.start()

    for k in range(3):
        over(k).start()
        twin(k).start()

    ones = jnp.ones((8, bk), low)

    def block(kv, rows, slot, q, strips, masked, first):
        k = kvs[kv, 0, rows, :]
        scores = [_dot(k, qbuf[q, n, at : at + wide, :], 1, 1) for n, at in strips]
        weights, keeps = [], []
        for (n, at), s, mask in zip(strips, scores, masked):
            c = slice(n * tokens + at, n * tokens + at + wide)
            if mask:
                ok = lax.broadcasted_iota(jnp.int32, (bk, wide), 1) >= lax.broadcasted_iota(jnp.int32, (bk, wide), 0)
                s = jnp.where(ok, s, HIDDEN)
            peak = s.max(axis=0, keepdims=True)
            if not first:
                old = top[slot, :, c]
                peak = jnp.maximum(old, peak)
                keeps.append(jnp.exp2((old - peak) * e))
            top[slot, :, c] = peak
            weights.append(jnp.exp2((s - peak) * e).astype(low))
        values = jnp.concatenate([kvs[kv, 1, rows, :].T, ones], axis=0)
        for i, ((n, at), p) in enumerate(zip(strips, weights)):
            c = slice(n * tokens + at, n * tokens + at + wide)
            new = _dot(values, p, 1, 0)
            mix[slot, :, c] = new if first else mix[slot, :, c] * keeps[i] + new

    everything = [(n, at) for n in range(g) for at in range(0, tokens, wide)]

    per = tokens // bk

    def whole(kv, slot, q, first=0, last=per, more=None):
        def step(j, _):
            at = kv if more is None else jnp.where(j < per, kv, more)
            block(at, pl.ds(pl.multiple_of(lax.rem(j, per) * bk, bk), bk), slot, q, everything, [False] * len(everything), False)

        lax.fori_loop(first, last, step, None)

    def fresh(slot):
        top[slot] = jnp.full((1, cols), NEG, jnp.float32)
        mix[slot] = jnp.zeros((d + 8, cols), jnp.float32)

    def own(h):
        slot = lax.rem(h, 2)
        load(q_hbm, h, slot).wait()
        kv_load(h).wait()

        @pl.when(h + 1 < heads)
        def _():
            load(q_hbm, h + 1, 1 - slot).start()

        for j in range(0, tokens, bk):
            strips = [(n, at) for n, at in everything if at >= j]
            block(h, pl.ds(j, bk), h, slot, strips, [at == j for _, at in strips], j == 0)

    each(own)

    def give(slot, out, far, lse_out=None, lse_far=None):
        for n, at in everything:
            c = slice(n * tokens + at, n * tokens + at + wide)
            total = mix[slot, d : d + 1, c]
            part = 1 / total
            lse = top[slot, :, c] * scale + jnp.log(total)
            if lse_out is not None:
                lbuf[lse_out, :, c] = lse
            if lse_far is not None:
                high = jnp.maximum(lse, flse[lse_far, :, c])
                a, b = jnp.exp(lse - high), jnp.exp(flse[lse_far, :, c] - high)
                part = part * a / (a + b)
                t = mix[slot, :d, c] * part + qbuf[far, n, at : at + wide, :].astype(jnp.float32).T * (b / (a + b))
            else:
                t = mix[slot, :d, c] * part
            obuf[out, n, at : at + wide, :] = t.T.astype(low)

    @pl.when(is_high)
    def _():
        load(q_hbm, carried, 1).start()

        @pl.when(me == 2)
        def _():
            one_first.wait_recv()
            for k in range(3):
                one_next(k).start()

        @pl.when(me == 3)
        def _():
            zero_first.wait_recv()
            zero_next.start()

        load(q_hbm, carried, 1).wait()
        whole(zero + 3 - me, carried, 1)

    def visits(h):
        @pl.when(odd)
        def _():
            load(q_hbm, h, 1).start()

        @pl.when(odd | ((me == 0) & (h < carried)))
        def _():
            near_copy(h).wait_recv()

        @pl.when(is_low & (h < carried))
        def _():
            q_copy(h).wait_recv()
            load(guest_hbm, h, 0).start()
            fresh(heads)
            load(guest_hbm, h, 0).wait()
            whole(h, heads, 0, 0, 2 * per, heads + h)

            @pl.when(h >= 2)
            def _():
                o_copy(h - 2).wait_send()
                l_copy(h - 2).wait_send()

            give(heads, lax.rem(h, 2), None, lse_out=lax.rem(h, 2))
            o_copy(h).start()
            l_copy(h).start()

        @pl.when(odd)
        def _():
            load(q_hbm, h, 1).wait()
            whole(heads + h, h, 1)

    each(visits)
    for k in range(3):
        over(k).wait_recv()
        twin(k + 3).start()

    @pl.when(is_low)
    def _():
        for h in range(carried - 2, carried):
            o_copy(h).wait_send()
            l_copy(h).wait_send()

    @pl.when(is_high)
    def _():
        load(q_hbm, carried, 1).start()
        load(q_hbm, carried, 1).wait()

    def rest(h):
        def piece(t, _):
            start, last_but_one, last = (h == 0) & (t == 0), (h == carried - 1) & (t == 0), h == carried

            @pl.when((me == 2) & start)
            def _():
                zero_next.wait_recv()

            for n, due in enumerate((last_but_one, last & (t == 0), last & (t == 1))):
                @pl.when((me == 3) & due)
                def _():
                    one_next(n).wait_recv()

            half, fourth = per // 2, per // 4
            begin = jnp.where((me == 3) & last, half + t * fourth, 0)
            end = jnp.where(me == 2, jnp.where(start, per, 0), jnp.where(last, half + (t + 1) * fourth, jnp.where(last_but_one, half, 0)))
            whole(zero + me - 2, carried, 1, begin, end)

        lax.fori_loop(0, 2, piece, None)

    def finals(h):
        @pl.when(is_high)
        def _():
            rest(h)

        @pl.when(h >= 2)
        def _():
            out_copy(h - 2).wait()

        @pl.when(is_low | (h == carried))
        def _():
            give(h, lax.rem(h, 2), None)

        @pl.when(is_high & (h < carried))
        def _():
            o_copy(h).wait_recv()
            l_copy(h).wait_recv()
            load(far_hbm, h, 0).start()
            load(far_hbm, h, 0).wait()
            give(h, lax.rem(h, 2), 0, lse_far=h)

        out_copy(h).start()

    each(finals)
    for k in range(6):
        twin(k).wait_recv()
        twin(k).wait_send()
    for k in range(3):
        over(k).wait_send()
    for h in range(heads - 2, heads):
        out_copy(h).wait()

    @pl.when(me < 3)
    def _():
        each(lambda h: near_copy(h).wait_send(), 0, nears)

    @pl.when(is_high)
    def _():
        each(lambda h: q_copy(h).wait_send(), 0, carried)

    @pl.when(me == 0)
    def _():
        zero_first.wait_send()

    @pl.when(me == 1)
    def _():
        one_first.wait_send()

    @pl.when(me == 2)
    def _():
        for k in range(3):
            one_next(k).wait_send()

    @pl.when(me == 3)
    def _():
        zero_next.wait_send()


def group_attention(q, kv, wo, bk=512):
    heads, g, tokens, d = q.shape
    dma = lambda n: pltpu.SemaphoreType.DMA((n,))
    anywhere = pl.BlockSpec(memory_space=pl.ANY)
    like = jax.ShapeDtypeStruct(q.shape, q.dtype)
    return pl.pallas_call(
        functools.partial(_group, scale=d**-0.5, bk=bk),
        in_specs=[anywhere] * 3,
        out_specs=[anywhere] * 4,
        out_shape=[like] * 3 + [jax.ShapeDtypeStruct(wo.shape, wo.dtype)],
        input_output_aliases={2: 3},
        scratch_shapes=[
            pltpu.VMEM((2 * heads + 2, 2, tokens, d), q.dtype),
            pltpu.VMEM((2, g, tokens, d), q.dtype),
            pltpu.VMEM((heads + 1, d + 8, g * tokens), jnp.float32),
            pltpu.VMEM((heads + 1, 1, g * tokens), jnp.float32),
            pltpu.VMEM((2, g, tokens, d), q.dtype),
            pltpu.VMEM((2, 1, g * tokens), jnp.float32),
            pltpu.VMEM((heads, 1, g * tokens), jnp.float32),
            dma(heads), dma(2), dma(heads), dma(heads), dma(heads), dma(heads), dma(heads), dma(heads), dma(heads), dma(heads), dma(2), dma(3), dma(3), dma(6), dma(6),
            pltpu.SemaphoreType.DMA, pltpu.SemaphoreType.DMA, dma(4), dma(4),
        ],
        compiler_params=pltpu.CompilerParams(collective_id=1, has_side_effects=True, vmem_limit_bytes=67043328),
        cost_estimate=pl.CostEstimate(flops=10 * heads * g * tokens * tokens * d, transcendentals=0, bytes_accessed=12 * heads * g * tokens * d),
    )(q, kv, wo)


def _finish(x_ref, seen_ref, own_ref, wo_ref, y_ref, wbuf, seen_s, sems):
    @pl.when(pl.program_id(0) == 0)
    def _():
        me, shard = lax.axis_index("sp"), own_ref.shape[0]
        size = wo_ref.shape[0] // shard
        copies = []
        for k in range(size):
            rows = pl.ds(pl.multiple_of(lax.rem(me + k, size) * shard, 32), shard)
            copies.append(pltpu.make_async_copy(wo_ref.at[rows] if k else own_ref, wbuf.at[rows], sems.at[k]))
        for c in copies:
            c.start()
        for c in copies:
            c.wait()

    at = 0
    for i in range(seen_ref.shape[0]):
        for n in range(seen_ref.shape[1]):
            seen_s[:, at : at + HEAD] = seen_ref[i, n]
            at += HEAD
    step = 512
    for c in range(0, y_ref.shape[1], step):
        y = _dot(seen_s[...], wbuf[:, c : c + step], 1, 0)
        y_ref[:, c : c + step] = (x_ref[:, c : c + step].astype(jnp.float32) + y).astype(jnp.bfloat16)


def finish(x, seen, own, wo, bm=256):
    tokens, d = x.shape
    k = wo.shape[0]
    row = lambda i: (i, 0)
    anywhere = pl.BlockSpec(memory_space=pl.ANY)
    return pl.pallas_call(
        _finish,
        grid=(tokens // bm,),
        in_specs=[pl.BlockSpec((bm, d), row), pl.BlockSpec((*seen.shape[:2], bm, HEAD), lambda i: (0, 0, i, 0)), anywhere, anywhere],
        out_specs=pl.BlockSpec((bm, d), row),
        scratch_shapes=[pltpu.VMEM((k, d), jnp.bfloat16), pltpu.VMEM((bm, k), jnp.bfloat16), pltpu.SemaphoreType.DMA((k // own.shape[0],))],
        out_shape=jax.ShapeDtypeStruct((tokens, d), jnp.bfloat16),
        compiler_params=pltpu.CompilerParams(dimension_semantics=("arbitrary",), vmem_limit_bytes=VMEM),
        cost_estimate=pl.CostEstimate(flops=2 * tokens * d * k, transcendentals=0, bytes_accessed=2 * (2 * tokens * d + d * k + 2 * tokens * k)),
    )(x, seen, own, wo)


def solution(mesh):
    size = mesh.shape["sp"]

    def step(x, gain, wq, wk, wv, wo):
        own = x.shape[0]
        half = HEAD // 2
        place = jnp.concatenate([lax.axis_index("sp") * own + jnp.arange(0, own, FINE), jnp.arange(FINE)])
        angle = place.astype(jnp.float32)[:, None] * THETA ** (-jnp.arange(half, dtype=jnp.float32) / half)
        turn = jnp.stack([jnp.cos(angle), jnp.sin(angle)])
        kv, q, wo_part = projections(x, gain[None], turn, wq, wk, wv, wo, size)
        seen, _, _, wo_whole = group_attention(q, kv, wo_part)
        return finish(x, seen, wo, wo_whole)

    tokens, whole = P(("dp", "sp"), None), P("sp", None)
    return jax.shard_map(
        step,
        mesh=mesh,
        in_specs=(tokens, P(None), whole, whole, whole, whole),
        out_specs=tokens,
        check_vma=False,
    )
```
